32 devices in a mesh: dp: 8 (over z, core), tp: 4 (over y, x).
Axes of the slice: x: 2, y: 2, z: 4, core: 2. Of those that a mesh axis runs over, the one named last changes fastest.
Arguments:
- tokens: bfloat16 [4096, 4096], P('dp'), may hold values from -6 to 6
- gain: float32 [4096], replicated, may hold values from 0.1 to 1.9
- router: float32 [4096, 8], replicated, may hold values from -0.09375 to 0.09375
- routes: int32 [4096, 2], P('dp'), may hold values from 0 to 7, all different within a row
- w_gate: bfloat16 [2, 4096, 1024], P(None, 'dp', 'tp'), may hold values from -0.125 to 0.125
- w_up: bfloat16 [2, 4096, 1024], P(None, 'dp', 'tp'), may hold values from -0.125 to 0.125
- w_down: bfloat16 [2, 1024, 4096], P(None, 'dp', 'tp'), may hold values from -0.25 to 0.25
Outputs:
- mixed: bfloat16 [4096, 4096], P('dp', 'tp')
The draws below stay inside these ranges and needn't reach their ends.
Inputs may be any that keep to these rules, and one draw needn't show every extreme that they name: `routes`: each row names two different experts.
All inputs are finite; a program needn't handle non-finite values.
Results may differ from the reference program's by a relative error of at most 0.0065.
Values may be sent and summed in bfloat16 or wider, within the bound.
A program may use at most 64 MiB of HBM per device.

```python
import jax
import jax.numpy as jnp
from jax import lax

D = 4096
FF = 1024
EXP = 2
ROUTED = 8
TOK_GRP = 512
TOKENS = 4096


def raised(array, own_key, source, target, blocks, factor):
    def block_of(axis_at):
        return (jnp.arange(array.shape[axis_at]) // (array.shape[axis_at] // blocks)).reshape((-1,) + (1,) * (array.ndim - 1 - axis_at))

    near = jax.random.permutation(own_key, blocks)[block_of(target)]
    second = (block_of(target) + blocks // 2) % blocks
    return jnp.where((block_of(source) == near) | (block_of(source) == second), factor * array, array)


def steps_of(rng, shape, shards, smallest, largest):
    level = 1.0
    for dim, blocks in shards:
        steps = jax.random.uniform(jax.random.fold_in(jax.random.fold_in(rng, 6), dim), (blocks,), jnp.float32, smallest / len(shards), largest / len(shards))
        level = level * jnp.repeat(jnp.exp(steps), shape[dim] // blocks).reshape((-1,) + (1,) * (len(shape) - 1 - dim))
    return level


def different_ones(rng, rows, amount, top, lift):
    sequence = jax.random.permutation(jax.random.fold_in(rng, 1), amount)
    favour = sequence
    for power in range(3):
        favour = favour * favour // amount
    favour = favour * lift // amount
    lots = jax.random.randint(jax.random.fold_in(rng, 2), (rows, amount), 0, 4096) + favour
    fixed_rows = jax.random.permutation(jax.random.fold_in(rng, 3), rows)[jnp.arange(amount) % rows]
    lots = jnp.where(jnp.arange(rows)[:, None] == fixed_rows[None, :], 1 << 14, lots)
    score = lots * amount + jnp.arange(amount)
    return lax.top_k(score.astype(jnp.int32), top)[1].astype(jnp.int32)


def noise(own_key, shape, deviation, reach, split=(), kind=jnp.bfloat16):
    level = steps_of(own_key, shape, split, -0.22, 0.18) if split else 1.0
    values = jax.random.normal(own_key, shape, jnp.float32) * deviation * level
    return jnp.minimum(jnp.maximum(values, -reach), reach).astype(kind)


def heavy_noise(rng, shape, width, most, cuts, heavy, kind=jnp.bfloat16):
    drawn = width * jax.random.normal(rng, shape, jnp.float32)
    if cuts:
        drawn = drawn * steps_of(rng, shape, cuts, -0.22, 0.18)
    return jnp.clip(raised(drawn, jax.random.fold_in(rng, 3), *heavy), -most, most).astype(kind)


def setup_inputs(seed: int = 0) -> dict:
    keys = jax.random.split(jax.random.key(seed), 8)
    return {
        "tokens": noise(keys[0], (TOKENS, D), 1.0, 6.0, ((0, 8),)),
        "gain": jnp.clip(1.0 + 0.18 * jax.random.normal(keys[1], (D,), jnp.float32), 0.1, 1.9),
        "router": noise(keys[2], (D, ROUTED), D ** -0.5, 0.09375, (), jnp.float32),
        "routes": different_ones(keys[3], TOKENS, ROUTED, 2, 2048),
        "w_gate": heavy_noise(keys[4], (EXP, D, FF), D ** -0.5, 0.125, ((1, 8), (2, 4)), (1, 2, 8, 2.0)),
        "w_up": heavy_noise(keys[5], (EXP, D, FF), D ** -0.5, 0.125, ((1, 8), (2, 4)), (1, 2, 8, 2.0)),
        "w_down": heavy_noise(keys[6], (EXP, FF, D), FF ** -0.5, 0.25, ((1, 8), (2, 4)), (1, 2, 8, 2.0)),
    }


EPS = 1e-06
ROUTE_SCALE = 2.5

def one_group(tokens, gain, router, routes, w_gate, w_up, w_down):
    values = tokens.astype(jnp.float32)
    square = lax.optimization_barrier(jnp.mean(values * values, axis=-1, keepdims=True))
    normed = (values * lax.rsqrt(square + EPS) * gain).astype(jnp.bfloat16)
    scores = jax.nn.sigmoid(jnp.dot(normed.astype(jnp.float32), router, precision=lax.Precision.HIGHEST))
    labels = jnp.arange(router.shape[1], dtype=jnp.int32)
    picked_mask = (routes[:, :, None] == labels[None, None, :]).astype(jnp.float32)
    picked = lax.optimization_barrier(jnp.sum(picked_mask * scores[:, None, :], axis=-1))
    chosen = lax.optimization_barrier(jnp.sum(picked_mask, axis=1))
    combine = chosen * scores * ROUTE_SCALE / lax.optimization_barrier(jnp.sum(picked, axis=-1, keepdims=True))
    total = jnp.zeros((tokens.shape[0], w_down.shape[2]), jnp.float32)
    for expert in range(w_gate.shape[0]):
        gate_value = jnp.dot(normed, w_gate[expert], preferred_element_type=jnp.float32)
        up_value = jnp.dot(normed, w_up[expert], preferred_element_type=jnp.float32)
        hidden = (jax.nn.silu(gate_value) * up_value * combine[:, expert:expert + 1]).astype(jnp.bfloat16)
        total = total + jnp.dot(hidden, w_down[expert], preferred_element_type=jnp.float32)
    return total.astype(jnp.bfloat16)

def reference(tokens, gain, router, routes, w_gate, w_up, w_down):
    groups = tokens.shape[0] // TOK_GRP
    grouped = tokens.reshape(groups, TOK_GRP, tokens.shape[1])
    grouped_routes = routes.reshape(groups, TOK_GRP, 2)

    def apply(pair):
        return one_group(pair[0], gain, router, pair[1], w_gate, w_up, w_down)
    mixed = lax.map(apply, (grouped, grouped_routes))
    return mixed.reshape(tokens.shape[0], w_down.shape[2])
```

```python
import functools

import jax
import jax.numpy as jnp
from jax import lax
from jax.experimental import pallas as pl
from jax.experimental.pallas import tpu as pltpu
from jax.sharding import PartitionSpec as P

EPS = 1e-06
ROUTE_SCALE = 2.5
MESH = pl.DeviceIdType.MESH
CORES = 2
PIECES = 8
CUTS = 2
HALVES = 2


def gathered(tokens, gain, router, routes, w_gate, w_up, w_down):
    values = tokens.astype(jnp.float32)
    square = jnp.mean(values * values, axis=-1, keepdims=True)
    normed = (values * lax.rsqrt(square + EPS) * gain).astype(jnp.bfloat16)
    scores = jax.nn.sigmoid(
        jnp.dot(normed.astype(jnp.float32), router, precision=lax.Precision.HIGHEST)
    )
    labels = jnp.arange(router.shape[1], dtype=jnp.int32)
    picked_mask = (routes[:, :, None] == labels[None, None, :]).astype(jnp.float32)
    picked = jnp.sum(picked_mask * scores[:, None, :], axis=-1)
    chosen = jnp.sum(picked_mask, axis=1)
    combine = chosen * scores * ROUTE_SCALE / jnp.sum(picked, axis=-1, keepdims=True)
    held_weights = combine[:, : w_gate.shape[0]]
    full_gate, full_up, full_down = (
        lax.all_gather(w_gate, "dp", axis=1, tiled=True),
        lax.all_gather(w_up, "dp", axis=1, tiled=True),
        lax.all_gather(w_down, "dp", axis=1, tiled=True),
    )
    gate_value = jnp.einsum("td,edf->tef", normed, full_gate, preferred_element_type=jnp.float32)
    up_value = jnp.einsum("td,edf->tef", normed, full_up, preferred_element_type=jnp.float32)
    hidden = (jax.nn.silu(gate_value) * up_value * held_weights[:, :, None]).astype(jnp.bfloat16)
    whole_hidden = lax.all_gather(hidden, "tp", axis=2, tiled=True)
    mixed = jnp.einsum("tef,efd->td", whole_hidden, full_down, preferred_element_type=jnp.float32)
    return mixed.astype(jnp.bfloat16)


def kernel(
    groups, tps, x_hbm, gain_hbm, router_hbm, routes_hbm, wg_hbm, wu_hbm, wd_hbm, o_ref,
    x, guest, guest_normed, w, dn, hid, guest_hid, comb, acc, gain_ref, router_ref, routes_ref,
    x_sem, own_sem, recv_sem, in_sem, out_sem, side_sem, hid_send, hid_recv,
    tok_send, tok_recv, back_send, back_recv,
):
    dp, tp = lax.axis_index("dp"), lax.axis_index("tp")
    positions = groups // CORES
    z, core = dp // CORES, dp % CORES
    experts = wg_hbm.shape[0]
    rows = x.shape[0]
    half = wg_hbm.shape[2] // HALVES
    end = jnp.logical_or(z == positions - 1, z == 0)
    out = 2 * (2 * z // positions) - 1

    def at(p):
        return (p * CORES + core, tp)

    inner = at(z - out)
    outer = at(jnp.clip(z + out, 0, positions - 1))
    side = (z * CORES + (1 - core), tp)
    along_x = tp + 1 - 2 * (tp % 2)
    along_y = lax.rem(tp + 2, tps)
    across = lax.rem(along_x + 2, tps)
    far = jnp.where(2 * z < positions, positions - 1, 0)
    others = [lax.rem(far + i, positions) for i in range(1, positions)]

    barrier = pltpu.get_barrier_semaphore()
    pl.semaphore_signal(barrier, inc=1, device_id=side, device_id_type=MESH)
    pl.semaphore_signal(barrier, inc=1, device_id=inner, device_id_type=MESH)
    for i in range(1, tps):
        pl.semaphore_signal(
            barrier, inc=1, device_id=(dp, lax.rem(tp + i, tps)), device_id_type=MESH
        )

    @pl.when(jnp.logical_not(end))
    def _():
        pl.semaphore_signal(barrier, inc=1, device_id=outer, device_id_type=MESH)

    loads = [
        pltpu.make_async_copy(src, dst, x_sem.at[i])
        for i, (src, dst) in enumerate(
            [(x_hbm, x), (gain_hbm, gain_ref), (router_hbm, router_ref), (routes_hbm, routes_ref)]
        )
    ]
    for load in loads:
        load.start()
    units = experts * HALVES
    feeds = list(range(2 * units))
    downs = list(range(2 * units, 2 * units + experts * CUTS))
    pieces = feeds + downs
    cut = wd_hbm.shape[1] // CUTS

    def source(k):
        if k < 2 * units:
            e, h = divmod(k // 2, HALVES)
            return (wg_hbm, wu_hbm)[k % 2].at[e, :, pl.ds(h * half, half)]
        e, r = divmod(k - 2 * units, CUTS)
        return wd_hbm.at[e, pl.ds(r * cut, cut), :]

    def slot(k, d):
        if k < 2 * units:
            return w.at[k // 2, k % 2, d]
        e, r = divmod(k - 2 * units, CUTS)
        return dn.at[e, d, pl.ds(r * cut, cut), :]

    def copy_own(k):
        return pltpu.make_async_copy(source(k), slot(k, dp), own_sem.at[k])

    for k in downs:
        copy_own(k).start()

    @pl.when(jnp.logical_not(end))
    def _():
        for k in feeds:
            copy_own(k).start()

    pl.semaphore_wait(barrier, tps + 2 - jnp.where(end, 1, 0))

    def send(k, d, src, sem, to):
        return pltpu.make_async_remote_copy(
            src_ref=src, dst_ref=slot(k, d), send_sem=sem.at[k, d // CORES],
            recv_sem=recv_sem.at[k, d], device_id=to, device_id_type=MESH,
        )

    def arrived(k, d):
        send(k, d, slot(k, d), side_sem, side).wait_recv()

    def pass_on(k, p, targets):
        d = p * CORES + core
        arrived(k, d)
        for sem, to in targets:
            send(k, d, slot(k, d), sem, to).start()

    def from_side(k, p):
        arrived(k, p * CORES + (1 - core))

    quarter = rows // tps
    piece = quarter // PIECES

    def token_part(q, p):
        return pl.ds(pl.multiple_of(q * quarter + p * piece, piece), piece)

    def token_copy(src, q, p, kind, to):
        return pltpu.make_async_remote_copy(
            src_ref=src.at[token_part(q, p)], dst_ref=guest.at[token_part(q, p)],
            send_sem=tok_send.at[kind, p], recv_sem=tok_recv.at[q, p],
            device_id=to, device_id_type=MESH,
        )

    def token_arrived(q, p):
        token_copy(guest, q, p, 0, side).wait_recv()

    def norm(src, dst, start, count, steps):
        step = count // steps

        def body(i, _):
            part = pl.ds(pl.multiple_of(start + i * step, step), step)
            v = src[part, :].astype(jnp.float32)
            square = jnp.mean(v * v, axis=-1, keepdims=True)
            dst[part, :] = (v * lax.rsqrt(square + EPS) * gain_ref[...]).astype(jnp.bfloat16)
            return 0

        lax.fori_loop(0, steps, body, 0)

    def norm_quarter(q):
        norm(guest, guest_normed, q * quarter, quarter, 2)

    def score():
        rest = router_ref[...]
        routed = rest.shape[0]
        parts = []
        for _ in range(3):
            part = rest.astype(jnp.bfloat16).astype(jnp.float32)
            rest = rest - part
            parts.append(part)
        parts.append(jnp.zeros_like(rest))
        stacked = jnp.concatenate(parts, axis=0).astype(jnp.bfloat16)
        sums = lax.dot_general(
            x[...], stacked, (((1,), (1,)), ((), ())), preferred_element_type=jnp.float32
        )
        total = sums[:, 2 * routed : 3 * routed] + sums[:, routed : 2 * routed] + sums[:, :routed]
        scores = 1.0 / (1.0 + jnp.exp(-total))
        picks = routes_ref[...].astype(jnp.float32)
        labels = lax.broadcasted_iota(jnp.int32, scores.shape, 1).astype(jnp.float32)
        chosen = jnp.zeros_like(scores)
        for i in range(routes_ref.shape[0]):
            column = jnp.transpose(jnp.broadcast_to(picks[i : i + 1, :], (128, rows)))
            chosen += jnp.where(column[:, :routed] == labels, 1.0, 0.0)
        picked = chosen * scores
        comb[...] = picked * ROUTE_SCALE / jnp.sum(picked, axis=-1, keepdims=True)

    def send_hidden(q, i):
        return pltpu.make_async_remote_copy(
            src_ref=hid.at[q, tp], dst_ref=hid.at[q, tp], send_sem=hid_send.at[q, i - 1],
            recv_sem=hid_recv.at[q, tp],
            device_id=(dp, lax.rem(tp + i, tps)), device_id_type=MESH,
        )

    def share_hidden(q):
        for i in range(1, tps):
            send_hidden(q, i).start()

    def hidden_arrived(q):
        for i in range(1, tps):
            s = lax.rem(tp + i, tps)
            pltpu.make_async_remote_copy(
                src_ref=hid.at[q, s], dst_ref=hid.at[q, s], send_sem=hid_send.at[q, i - 1],
                recv_sem=hid_recv.at[q, s], device_id=side, device_id_type=MESH,
            ).wait_recv()

    def send_back(q):
        return pltpu.make_async_remote_copy(
            src_ref=guest_hid.at[q], dst_ref=hid.at[q, tp], send_sem=back_send.at[q],
            recv_sem=back_recv.at[q], device_id=outer, device_id_type=MESH,
        )

    def unit_hidden(q, src, dst):
        depth = x.shape[1]
        step = rows // 2

        def body(i, _):
            part = pl.ds(pl.multiple_of(i * step, step), step)
            weights = jnp.concatenate(
                [w[q, 0].reshape(depth, half), w[q, 1].reshape(depth, half)], axis=1
            )
            both = jnp.dot(src[part, :], weights, preferred_element_type=jnp.float32)
            gate, up = both[:, :half], both[:, half:]
            dst[part, :] = (gate / (1.0 + jnp.exp(-gate)) * up).astype(jnp.bfloat16)
            return 0

        lax.fori_loop(0, 2, body, 0)

    def own_hidden(q):
        unit_hidden(q, x, hid.at[q, tp])
        share_hidden(q)

    def guest_hidden(q):
        unit_hidden(q, guest_normed, guest_hid.at[q])
        send_back(q).start()

    def sides_of(q):
        for k in (2 * q, 2 * q + 1):
            for p in range(positions):
                from_side(k, p)
            copy_own(k).wait()

    def down(terms, first, last):
        cols = o_ref.shape[1]
        step = cols // 4

        def body(i, _):
            part = pl.ds(pl.multiple_of(i * step, step), step)
            total = None if first else acc[:, part]
            for e, spots in terms:
                lhs = jnp.concatenate(
                    [hid[e * HALVES + h, t] for t in spots for h in range(HALVES)], axis=1
                )
                rhs = jnp.concatenate(
                    [
                        dn[e, pl.ds(t * CORES, CORES), :, part].reshape(HALVES * half, step)
                        for t in spots
                    ],
                    axis=0,
                )
                term = jnp.dot(lhs, rhs, preferred_element_type=jnp.float32)
                term = term * comb[:, e : e + 1]
                total = term if total is None else total + term
            if last:
                o_ref[:, part] = total.astype(o_ref.dtype)
            else:
                acc[:, part] = total
            return 0

        lax.fori_loop(0, 4, body, 0)

    def down_near(e):
        for q in range(e * HALVES, (e + 1) * HALVES):
            hidden_arrived(q)
        for k in downs[e * CUTS : (e + 1) * CUTS]:
            for p in others:
                from_side(k, p)
            copy_own(k).wait()
        down([(e, others)], e == 0, False)

    to_in, to_out, to_side = (in_sem, inner), (out_sem, outer), (side_sem, side)

    @pl.when(end)
    def _():
        for p in range(PIECES):
            token_copy(x_hbm, tp, p, 0, inner).start()
        for k in pieces:
            send(k, dp, source(k), *to_in).start()
        for k in downs:
            send(k, dp, source(k), *to_side).start()
        for load in loads:
            load.wait()
        norm(x, x, 0, rows, 8)
        score()
        for j in range(1, positions - 1):
            for k in downs:
                pass_on(k, z - j * out, [to_side])
        for q in range(units):
            send_back(q).wait_recv()
            share_hidden(q)
            if q == units - 2:
                down_near(0)
        for k in downs[:-1]:
            pass_on(k, far, [to_side])
        down_near(1)
        pass_on(downs[-1], far, [to_side])

    @pl.when(jnp.logical_not(end))
    def _():
        for k in pieces:
            send(k, dp, source(k), *to_in).start()
        for k in downs:
            send(k, dp, source(k), *to_out).start()
        for k in pieces:
            send(k, dp, source(k), *to_side).start()

        def beyond(k):
            return [to_out] if k in downs else []

        def from_outer(k):
            pass_on(k, z + out, [to_in, to_side])

        def from_near(k):
            pass_on(k, z - out, beyond(k) + [to_side])

        def from_far(k):
            pass_on(k, far, beyond(k) + [to_side])

        for load in loads:
            load.wait()
        norm(x, x, 0, rows, 8)
        for p in range(PIECES):
            token_arrived(tp, p)
            token_copy(guest, tp, p, 0, (dp, along_x)).start()
            token_copy(guest, tp, p, 1, (dp, along_y)).start()
            from_near(feeds[p])
            if p == 1:
                score()
        for p in range(PIECES // 2):
            token_arrived(along_x, p)
            token_copy(guest, along_x, p, 2, (dp, along_y)).start()
            token_arrived(along_y, p + PIECES // 2)
            token_copy(guest, along_y, p + PIECES // 2, 2, (dp, along_x)).start()
        norm_quarter(tp)
        for i in range(4):
            from_outer(feeds[i])
            from_near(downs[i])
            if i == 0:
                for p in range(PIECES // 2):
                    token_arrived(along_x, p + PIECES // 2)
                    token_arrived(along_y, p)
                norm_quarter(along_x)
            if i == 1:
                norm_quarter(along_y)
        from_far(feeds[0])
        from_outer(feeds[4])
        for p in range(PIECES):
            token_arrived(across, p)
        norm_quarter(across)
        from_far(feeds[1])
        from_outer(feeds[5])
        late = feeds[6:] + downs
        for q in range(units):
            sides_of(q)
            guest_hidden(q)
            own_hidden(q)
            for i in (2 * q, 2 * q + 1):
                if i + 2 < len(feeds):
                    from_far(feeds[i + 2])
                if i < len(late):
                    from_outer(late[i])
        down_near(0)
        for k in downs[:-1]:
            from_far(k)
        down_near(1)
        from_far(downs[-1])

    for k in downs:
        from_side(k, far)
    down([(e, [far]) for e in range(experts)], False, True)

    def sent(k, p, sem):
        d = p * CORES + core
        send(k, d, slot(k, d), sem, side).wait_send()

    for q in range(units):
        for i in range(1, tps):
            send_hidden(q, i).wait_send()
    for k in pieces:
        sent(k, z, in_sem)

    @pl.when(end)
    def _():
        for p in range(PIECES):
            token_copy(x_hbm, tp, p, 0, inner).wait_send()
        for k in downs:
            for p in range(positions):
                sent(k, p, side_sem)

    @pl.when(jnp.logical_not(end))
    def _():
        for p in range(PIECES):
            for kind in range(2):
                token_copy(guest, tp, p, kind, side).wait_send()
            token_copy(guest, tp, p, 2, side).wait_send()
        for q in range(units):
            send_back(q).wait_send()
        for k in pieces:
            sent(k, z + out, in_sem)
            for p in range(positions):
                sent(k, p, side_sem)
        for k in downs:
            sent(k, z, out_sem)
            sent(k, z - out, out_sem)
            sent(k, far, out_sem)


def streamed(groups, tps, tokens, gain, router, routes, w_gate, w_up, w_down):
    rows, depth = tokens.shape
    experts, shard, width = w_gate.shape
    down_rows, cols = w_down.shape[1:]
    positions = groups // CORES
    half = width // HALVES
    if down_rows != half or half % 128:
        return gathered(tokens, gain, router, routes, w_gate, w_up, w_down)
    hbm = pl.BlockSpec(memory_space=pltpu.HBM)
    units = experts * HALVES
    pieces = 2 * units + experts * CUTS
    dma = pltpu.SemaphoreType.DMA
    return pl.pallas_call(
        functools.partial(kernel, groups, tps),
        out_shape=pltpu.VMEM((rows, cols), jnp.bfloat16),
        in_specs=[hbm] * 7,
        out_specs=pl.BlockSpec(memory_space=pltpu.VMEM),
        scratch_shapes=[
            pltpu.VMEM((rows, depth), jnp.bfloat16),
            pltpu.VMEM((rows, depth), jnp.bfloat16),
            pltpu.VMEM((rows, depth), jnp.bfloat16),
            pltpu.VMEM((units, 2, groups, shard, half), jnp.bfloat16),
            pltpu.VMEM((experts, groups, down_rows, cols), jnp.bfloat16),
            pltpu.VMEM((units, tps, rows, half), jnp.bfloat16),
            pltpu.VMEM((units, rows, half), jnp.bfloat16),
            pltpu.VMEM((rows, router.shape[1]), jnp.float32),
            pltpu.VMEM((rows, cols), jnp.float32),
            pltpu.VMEM((1, depth), jnp.float32),
            pltpu.VMEM((router.shape[1], depth), jnp.float32),
            pltpu.VMEM((routes.shape[1], rows), jnp.int32),
            dma((4,)),
            dma((pieces,)),
            dma((pieces, groups)),
            dma((pieces, positions)),
            dma((pieces, positions)),
            dma((pieces, positions)),
            dma((units, tps - 1)),
            dma((units, tps)),
            dma((3, PIECES)),
            dma((tps, PIECES)),
            dma((units,)),
            dma((units,)),
        ],
        compiler_params=pltpu.CompilerParams(
            collective_id=0, has_side_effects=True, vmem_limit_bytes=60 * 1024 * 1024
        ),
    )(tokens, gain.reshape(1, -1), router.T, routes.T, w_gate, w_up, w_down)


def solution(mesh):
    groups, tps = mesh.shape["dp"], mesh.shape["tp"]
    fits = groups == 4 * CORES and tps == 4
    body = functools.partial(streamed, groups, tps) if fits else gathered
    return jax.shard_map(
        body,
        mesh=mesh,
        in_specs=(
            P("dp", None),
            P(),
            P(),
            P("dp", None),
            P(None, "dp", "tp"),
            P(None, "dp", "tp"),
            P(None, "dp", "tp"),
        ),
        out_specs=P("dp", "tp"),
        check_vma=False,
    )
```
